32 devices in a mesh: row: 4 (over y, x), col: 8 (over z, core).
Axes of the slice: x: 2, y: 2, z: 4, core: 2. Of those that a mesh axis runs over, the one named last changes fastest.
Arguments:
- points: bfloat16 [10240, 64], P(('row', 'col')), may hold values from -5 to 5
- start_vectors: bfloat16 [10240, 32], P(('row', 'col')), may hold values from -12 to 12
Outputs:
- basis: float32 [10240, 32], P(('row', 'col'))
The draws below stay inside these ranges and needn't reach their ends.
All inputs are finite; a program needn't handle non-finite values.
Results may differ from the reference program's by a relative error of at most 0.007.
Values may be sent and summed in bfloat16 or wider, within the bound.
A program may use at most 64 MiB of HBM per device.

```python
import jax
import jax.numpy as jnp
from jax import lax

F = 64
K = 32
ITERS = 2
PTS_BLK = 2560
POINTS = 10240


def draw_points(key, part):
    order_key, center_key, noise_key, sigma_key = jax.random.split(jax.random.fold_in(key, 11), 4)
    pairs = POINTS // 2
    order = jax.random.permutation(order_key, POINTS)
    pair_of = jnp.zeros((POINTS,), jnp.int32).at[order].set(jnp.arange(POINTS, dtype=jnp.int32) // 2)
    sigma = jnp.exp(jax.random.uniform(sigma_key, (pairs, 1), jnp.float32, jnp.log(0.15), jnp.log(0.4)))
    centers = jnp.clip(jax.random.normal(center_key, (pairs, F), jnp.float32), -4.0, 4.0)
    noise = jnp.clip(jax.random.normal(noise_key, (POINTS, F), jnp.float32), -3.0, 3.0)
    values = centers[pair_of] + sigma[pair_of] * noise
    return jnp.clip(values, -5.0, 5.0).astype(jnp.bfloat16)


def draw_start_vectors(key, part):
    position = jnp.arange(POINTS, dtype=jnp.float32)[:, None] / POINTS
    base = jnp.clip(jax.random.normal(key, (POINTS, K), jnp.float32), -3.0, 3.0)
    values = base * jnp.exp(jnp.log(4.0) * position)
    return jnp.clip(values, -12.0, 12.0).astype(jnp.bfloat16)


def setup_inputs(seed: int = 0) -> dict:
    key_of = jax.random.split(jax.random.key(seed), 3)
    return {
        "points": draw_points(jax.random.fold_in(key_of[2], 71), 0),
        "start_vectors": draw_start_vectors(jax.random.fold_in(key_of[2], 71), 0),
    }


KERNEL_SCALE = 5.12

def kernel_block(block_pts, block_sq, all_pts, all_sq):
    cross = jnp.dot(block_pts.astype(jnp.float32), all_pts.T.astype(jnp.float32), preferred_element_type=jnp.float32)
    dist = block_sq[:, None] + all_sq[None, :] - 2.0 * cross
    return jnp.exp(dist * (-KERNEL_SCALE / F)).astype(jnp.bfloat16)

def reference(points, start_vectors):
    sq_norms = jnp.sum(jnp.square(points.astype(jnp.float32)), axis=1)
    height = min(512, PTS_BLK)
    count = POINTS // height
    stacked = (points.reshape(count, height, F), sq_norms.reshape(count, height))

    def degree_block(item):
        weights = kernel_block(item[0], item[1], points, sq_norms)
        return jnp.sum(weights, axis=1, dtype=jnp.float32)
    degree = lax.map(degree_block, stacked).reshape(POINTS)
    vectors = start_vectors
    ortho = jnp.zeros((POINTS, K), jnp.float32)
    for step in range(ITERS):

        def product_block(item, panel=vectors):
            weights = kernel_block(item[0], item[1], points, sq_norms)
            return jnp.dot(weights.astype(jnp.float32), panel.astype(jnp.float32), preferred_element_type=jnp.float32)
        product = lax.map(product_block, stacked).reshape(POINTS, K)
        scaled = product / degree[:, None]
        gram = jnp.dot(scaled.T.astype(jnp.float32), scaled.astype(jnp.float32), precision=lax.Precision.HIGHEST, preferred_element_type=jnp.float32) / POINTS
        lower = jnp.linalg.cholesky(gram)
        ortho = lax.linalg.triangular_solve(lower, scaled, left_side=False, lower=True, transpose_a=True)
        vectors = ortho.astype(jnp.bfloat16)
    return ortho
```

```python
import functools

import jax
import jax.numpy as jnp
from jax import lax
from jax.experimental import pallas as pl
from jax.experimental.pallas import tpu as pltpu
from jax.sharding import PartitionSpec as P

KERNEL_SCALE = 5.12
LOG2E = 1.4426950408889634
MESH = pl.DeviceIdType.MESH
HIGHEST = lax.Precision.HIGHEST
LANES = 128
ONES = 16
ROWS_OF = 8


def square_side(count):
    side = 1
    while side * side < count:
        side += 1
    return side if side * side == count else count


def upright(value):
    return value.astype(jnp.float32).T.astype(value.dtype)


def tail_stacks(vectors, rows):
    rest = rows % LANES
    if rest and LANES % rest == 0 and vectors % (LANES // rest * 16) == 0:
        return LANES // rest
    return 1


def packed_rows(vectors, rows):
    full, rest = rows // LANES, rows % LANES
    return full * vectors + (vectors // tail_stacks(vectors, rows) if rest else 0)


def pack(value):
    vectors, rows = value.shape
    full, rest = rows // LANES, rows % LANES
    pieces = [value[:, f * LANES : (f + 1) * LANES] for f in range(full)]
    if rest:
        tail = value[:, full * LANES :]
        stacks = tail_stacks(vectors, rows)
        tall = vectors // stacks
        parts = [tail[s * tall : (s + 1) * tall] for s in range(stacks)]
        spare = LANES - stacks * rest
        if spare:
            parts.append(jnp.zeros((tall, spare), value.dtype))
        pieces.append(jnp.concatenate(parts, axis=1))
    return jnp.concatenate(pieces, axis=0)


def unpack(value, vectors, rows):
    full, rest = rows // LANES, rows % LANES
    pieces = [value[f * vectors : (f + 1) * vectors] for f in range(full)]
    if rest:
        tail = value[full * vectors :]
        stacks = tail_stacks(vectors, rows)
        pieces.append(jnp.concatenate([tail[:, s * rest : (s + 1) * rest] for s in range(stacks)], axis=0))
    return jnp.concatenate(pieces, axis=1)


def inverse_factor(gram):
    size = gram.shape[0]
    down = lax.broadcasted_iota(jnp.int32, (size, size), 0)
    across = lax.broadcasted_iota(jnp.int32, (size, size), 1)
    unit = (down == across).astype(jnp.float32)
    work = jnp.concatenate([gram, unit], axis=1)
    below = lax.broadcasted_iota(jnp.int32, work.shape, 0)
    panel = 8
    for first in range(0, size, panel):
        columns = [jnp.broadcast_to(work[:, k : k + 1], work.shape) for k in range(first, first + panel)]
        for m in range(panel):
            k = first + m
            factor = jnp.where(below > k, columns[m] * (1.0 / columns[m][k : k + 1]), 0.0)
            work = work - factor * work[k : k + 1]
            for later in range(m + 1, panel):
                columns[later] = columns[later] - factor * columns[later][k : k + 1]
    pivots = jnp.sum(work[:, :size] * unit, axis=1, keepdims=True)
    return work[:, size:] * lax.rsqrt(pivots)


def kernel(nrow, ncol, total, pts_ref, vec_ref, out_ref, pair, gp, gv, gx, aff, acc, mine, theirs, gram1, gram2,
           recv_p, recv_v, recv_x, send_g, sems_d):
    row, col = lax.axis_index("row"), lax.axis_index("col")
    nz = ncol // 2
    z, core = col // 2, col % 2
    sibling = (row, z * 2 + (1 - core))
    features, rows = pts_ref.shape
    vectors = vec_ref.shape[0]
    chips = nrow * nz
    both = 2 * rows
    half = rows // 2
    side = square_side(nrow)
    high_row, low_row = row // side, row % side
    lesser = jnp.minimum(z, nz - 1 - z)
    upward = z < nz - 1 - z
    contract = (((1,), (1,)), ((), ()))

    def row_at(j):
        if j == 0:
            return row
        return lax.rem(high_row + j // side, nrow // side) * side + lax.rem(low_row + j % side, side)

    straight = [j for j in range(1, nrow) if j // side == 0 or j % side == 0]
    oblique = [j for j in range(1, nrow) if j // side and j % side]

    def z_at(m):
        if m == 0:
            return z
        q = m - 1
        near = z + (q // 2 + 1) * (1 if q % 2 else -1)
        step = q - lesser + 1
        far = jnp.where(upward, z + step, z - step)
        return jnp.where(q < 2 * lesser, near, far)

    levels = [z_at(m) for m in range(nz)]
    places = [row_at(j) for j in range(nrow)]

    def chip_at(j, m):
        return places[j] * nz + levels[m]

    def block(gather, j, m, to_row, to_z):
        buf, recv, send, routed = gather
        chip = chip_at(j, m)
        return pltpu.make_async_remote_copy(
            src_ref=buf.at[chip], dst_ref=buf.at[chip], send_sem=send_g.at[send], recv_sem=recv.at[chip],
            device_id=(to_row, to_z * 2 + core), device_id_type=MESH,
        )

    def arrived(gather, j, m):
        block(gather, j, m, row, z).wait_recv()

    def spread(gather, m):
        routed = gather[3]
        for j in straight + (oblique if routed else []):
            block(gather, 0, m, places[j], z).start()

    def send_own(gather):
        spread(gather, 0)
        for m in range(1, nz):
            block(gather, 0, 0, row, levels[m]).start()

    def pass_on(gather, m):
        arrived(gather, 0, m)
        spread(gather, m)

    def relay(gather, m):
        routed = gather[3]
        for j in straight:
            arrived(gather, j, m)
            if routed:
                continue
            if j // side == 0 and m % 2 == 0:
                targets = [d * side for d in range(1, nrow // side)]
            elif j % side == 0 and m % 2 == 1:
                targets = range(1, side)
            else:
                targets = []
            for t in targets:
                block(gather, j, m, places[t], z).start()

    def drain(gather):
        buf, recv, send, routed = gather
        sent = buf.at[pl.ds(0, chips - 1)]
        pltpu.make_async_remote_copy(
            src_ref=sent, dst_ref=sent, send_sem=send_g.at[send], recv_sem=recv.at[0],
            device_id=(row, col), device_id_type=MESH,
        ).wait_send()

    def swap(src, dst, n):
        return pltpu.make_async_remote_copy(
            src_ref=src, dst_ref=dst, send_sem=sems_d.at[2 * n], recv_sem=sems_d.at[2 * n + 1],
            device_id=sibling, device_id_type=MESH,
        )

    points = (gp, recv_p, 0, False)
    start = (gv, recv_v, 1, False)
    middle = (gx, recv_x, 2, True)

    barrier = pltpu.get_barrier_semaphore()
    for j in range(1, nrow):
        pl.semaphore_signal(barrier, inc=1, device_id=(places[j], col), device_id_type=MESH)
    for m in range(1, nz):
        pl.semaphore_signal(barrier, inc=1, device_id=(row, levels[m] * 2 + core), device_id_type=MESH)
    pl.semaphore_signal(barrier, inc=1, device_id=sibling, device_id_type=MESH)

    own = chip_at(0, 0)
    x = upright(pts_ref[...])
    gp[own] = jnp.concatenate([x[:half], x[half:]], axis=1)
    gv[own] = pack(vec_ref[...])
    with jax.named_scope("barrier"):
        pl.semaphore_wait(barrier, nrow + nz - 1)

    swap_points = swap(pts_ref, pair, 0)
    swap_points.start()
    send_own(points)
    send_own(start)

    rate = -KERNEL_SCALE / features * LOG2E
    with jax.named_scope("prep"):
        swap_points.wait()
        ours, other = pts_ref[...].astype(jnp.float32), pair[...].astype(jnp.float32)
        first_core = core == 0
        lane_points = jnp.concatenate(
            [jnp.where(first_core, ours, other), jnp.where(first_core, other, ours)], axis=1
        )
        here = jnp.sum(lane_points * lane_points, axis=0, keepdims=True) * rate
        lane_points = lane_points.astype(jnp.bfloat16)
        blank = jnp.zeros_like(lane_points)
        right = [
            jnp.concatenate([lane_points, blank], axis=0),
            jnp.concatenate([blank, lane_points], axis=0),
        ]
        lane = lax.broadcasted_iota(jnp.int32, (2 * LANES, 2 * LANES), 1)
        down = lax.broadcasted_iota(jnp.int32, (2 * LANES, 2 * LANES), 0)
        picks = (lax.rem(down, LANES) // features == lane // LANES).astype(jnp.bfloat16)

    def weights(j, m):
        left = gp[chip_at(j, m)]
        wide = left.astype(jnp.float32)
        square = wide * wide
        upper = square.astype(jnp.bfloat16)
        lower = (square - upper.astype(jnp.float32)).astype(jnp.bfloat16)
        there = jnp.dot(
            jnp.concatenate([upper, lower], axis=1), picks, preferred_element_type=jnp.float32
        ) * rate
        for t in range(2):
            cross = jnp.dot(left, right[t], preferred_element_type=jnp.float32)
            tile = there[:, t * LANES : (t + 1) * LANES]
            tiles = jnp.concatenate([tile] * (-(-both // LANES)), axis=1)[:, :both]
            power = (cross * (-2.0 * rate) + tiles) + here
            aff[j * nz + m, t * half : (t + 1) * half, :] = jnp.exp2(power).astype(jnp.bfloat16)

    counter = jnp.ones((ONES, rows), jnp.bfloat16)

    def first_product(blocks):
        part = 0.0
        for j, m in blocks:
            panel = jnp.concatenate([unpack(gv[chip_at(j, m)], vectors, rows), counter], axis=0)
            part = part + jnp.dot(panel, aff[j * nz + m], preferred_element_type=jnp.float32)
        return part

    with jax.named_scope("w_own"):
        weights(0, 0)
    for m in range(1, nz):
        with jax.named_scope(f"pass_p{m}"):
            pass_on(points, m)
            relay(points, m - 1)
        with jax.named_scope(f"w{m}"):
            weights(0, m)
            for j in straight:
                weights(j, m - 1)
        with jax.named_scope(f"pass_v{m}"):
            pass_on(start, m)
            relay(start, m - 1)
        if m > 1:
            for j in oblique:
                with jax.named_scope(f"wait_o{m - 2}"):
                    arrived(points, j, m - 2)
                with jax.named_scope(f"wo{m - 2}"):
                    weights(j, m - 2)
    with jax.named_scope("relay_p_last"):
        relay(points, nz - 1)
    with jax.named_scope("w_last"):
        for j in straight:
            weights(j, nz - 1)
    with jax.named_scope("first_a"):
        acc[...] = first_product([(0, m) for m in range(nz)] + [(j, m) for j in straight for m in range(nz - 1)])
    with jax.named_scope("relay_v_last"):
        relay(start, nz - 1)
    with jax.named_scope("first_b"):
        acc[...] += first_product([(j, nz - 1) for j in straight])
    for j in oblique:
        for m in range(max(0, nz - 2), nz):
            with jax.named_scope(f"wait_o{m}"):
                arrived(points, j, m)
            with jax.named_scope(f"wo{m}"):
                weights(j, m)
    with jax.named_scope("wait_vo"):
        for j in oblique:
            for m in range(nz):
                arrived(start, j, m)
    with jax.named_scope("first_c"):
        mine[...] = (acc[...] + first_product([(j, m) for j in oblique for m in range(nz)]))[: vectors + ROWS_OF]
    swap_first = swap(mine, theirs.at[0], 1)
    swap_first.start()
    with jax.named_scope("swap1"):
        swap_first.wait()

    with jax.named_scope("scale_send"):
        whole = mine[...] + theirs[0]
        degree = whole[vectors : vectors + 1]
        scaled = whole[:vectors] / degree
        ours = jnp.where(first_core, scaled[:, :rows], scaled[:, rows:])
        gx[own] = pack(ours.astype(jnp.bfloat16))
        send_own(middle)

    def second_product(blocks):
        part, cross = 0.0, 0.0
        for j, m in blocks:
            panel = unpack(gx[chip_at(j, m)], vectors, rows)
            part = part + jnp.dot(panel, aff[j * nz + m], preferred_element_type=jnp.float32)
            cross = cross + lax.dot_general(panel, panel, contract, preferred_element_type=jnp.float32)
        return part, cross

    with jax.named_scope("second_own"):
        part, cross = second_product([(0, 0)])
        acc[:vectors] = part
    for m in range(1, nz):
        with jax.named_scope(f"pass_x{m}"):
            pass_on(middle, m)
            relay(middle, m - 1)
        with jax.named_scope(f"second{m}"):
            part, more = second_product([(0, m)] + [(j, m - 1) for j in straight])
            acc[:vectors] += part
            cross = cross + more
    with jax.named_scope("relay_x_last"):
        relay(middle, nz - 1)
    with jax.named_scope("second_last"):
        part, more = second_product([(j, nz - 1) for j in straight])
        acc[:vectors] += part
        cross = cross + more
    with jax.named_scope("wait_xo"):
        for j in oblique:
            for m in range(nz):
                arrived(middle, j, m)
    with jax.named_scope("second_o"):
        part, more = second_product([(j, m) for j in oblique for m in range(nz)])
        gram1[0] = cross + more
        swap_gram = swap(gram1.at[0], gram1.at[1], 2)
        swap_gram.start()
        mine[:vectors] = acc[:vectors] + part
        swap_second = swap(mine.at[pl.ds(0, vectors)], theirs.at[1, pl.ds(0, vectors)], 3)
        swap_second.start()
    with jax.named_scope("swap_gram"):
        swap_gram.wait()
    with jax.named_scope("factor1"):
        first = inverse_factor((gram1[0] + gram1[1]) * (1.0 / total))
    with jax.named_scope("swap2"):
        swap_second.wait()
    folds = LANES // vectors
    tall = vectors // folds
    with jax.named_scope("gram2"):
        ratio = (mine[:vectors] + theirs[1, :vectors]) / degree
        scaled = jnp.dot(first, ratio, precision=HIGHEST, preferred_element_type=jnp.float32)
        part = lax.dot_general(
            scaled, scaled, contract, precision=HIGHEST, preferred_element_type=jnp.float32
        ) * (1.0 / total)
        gram2[own] = jnp.concatenate([part[f * tall : (f + 1) * tall] for f in range(folds)], axis=1)

    def gram_copy(j, m, to_row, to_z):
        chip = chip_at(j, m)
        return pltpu.make_async_remote_copy(
            src_ref=gram2.at[chip], dst_ref=gram2.at[chip], send_sem=sems_d.at[8], recv_sem=sems_d.at[9],
            device_id=(to_row, to_z * 2 + core), device_id_type=MESH,
        )

    with jax.named_scope("gram_send"):
        for m in reversed(range(nz)):
            for j in reversed(range(nrow)):
                if j or m:
                    gram_copy(0, 0, places[j], levels[m]).start()
        ours = jnp.where(first_core, scaled[:, :rows], scaled[:, rows:])
        drain(points)
        drain(start)
        drain(middle)
        sent = gram2.at[pl.ds(0, chips - 1)]
    with jax.named_scope("gram_wait"):
        pltpu.make_async_remote_copy(
            src_ref=sent, dst_ref=sent, send_sem=sems_d.at[8], recv_sem=sems_d.at[9],
            device_id=(row, col), device_id_type=MESH,
        ).wait()
    with jax.named_scope("factor2"):
        flat = jnp.sum(gram2[...], axis=0)
        gram = jnp.concatenate([flat[:, f * vectors : (f + 1) * vectors] for f in range(folds)], axis=0)
        second = inverse_factor(gram)
    with jax.named_scope("out"):
        out_ref[...] = jnp.dot(second, ours, precision=HIGHEST, preferred_element_type=jnp.float32)


def solution(mesh):
    nrow, ncol = mesh.shape["row"], mesh.shape["col"]
    nz = ncol // 2
    chips = nrow * nz

    def step(points, start_vectors):
        rows, features = points.shape
        vectors = start_vectors.shape[1]
        high = packed_rows(vectors, rows)
        dma = pltpu.SemaphoreType.DMA
        return pl.pallas_call(
            functools.partial(kernel, nrow, ncol, rows * nrow * ncol),
            out_shape=jax.ShapeDtypeStruct((vectors, rows), jnp.float32),
            in_specs=[pl.BlockSpec(memory_space=pltpu.VMEM)] * 2,
            out_specs=pl.BlockSpec(memory_space=pltpu.VMEM),
            scratch_shapes=[
                pltpu.VMEM((features, rows), jnp.bfloat16),
                pltpu.VMEM((chips, rows // 2, 2 * features), jnp.bfloat16),
                pltpu.VMEM((chips, high, LANES), jnp.bfloat16),
                pltpu.VMEM((chips, high, LANES), jnp.bfloat16),
                pltpu.VMEM((chips, rows, 2 * rows), jnp.bfloat16),
                pltpu.VMEM((vectors + ONES, 2 * rows), jnp.float32),
                pltpu.VMEM((vectors + ROWS_OF, 2 * rows), jnp.float32),
                pltpu.VMEM((2, vectors + ROWS_OF, 2 * rows), jnp.float32),
                pltpu.VMEM((2, vectors, vectors), jnp.float32),
                pltpu.VMEM((chips, vectors * vectors // LANES, LANES), jnp.float32),
                dma((chips,)), dma((chips,)), dma((chips,)), dma((3,)), dma((10,)),
            ],
            compiler_params=pltpu.CompilerParams(
                collective_id=0, has_side_effects=True, vmem_limit_bytes=56 * 1024 * 1024
            ),
        )(points.T, start_vectors.T).T

    return jax.shard_map(
        step,
        mesh=mesh,
        in_specs=(P(("row", "col"), None), P(("row", "col"), None)),
        out_specs=P(("row", "col"), None),
        check_vma=False,
    )
```
